512 devices in a mesh: gx: 32 (over z, core), gy: 16 (over x, y).
Axes of the slice: x: 4, y: 4, z: 16, core: 2. Of those that a mesh axis runs over, the one named last changes fastest.
Arguments:
- load: float32 [32, 16, 320, 768], P('gx', 'gy'), may hold values from -6 to 6
- stiffness: bfloat16 [32, 16, 768, 768], P('gx', 'gy'), may hold values from -0.5 to 3, as said below
- local_inverse: bfloat16 [32, 16, 768, 768], P('gx', 'gy'), may hold values from -0.5 to 3, as said below
- phi: float32 [32, 16, 8, 768], P('gx', 'gy'), may hold values from -2.5 to 2.5
- level2_inverse: float32 [32, 128, 128], P('gx'), may hold values from -0.5 to 3, as said below
- level3_inverse: bfloat16 [512, 512], replicated, may hold values from -0.5 to 3, as said below
- aggregate: int32 [32, 16], P('gx', 'gy'), may hold values from 0 to 1
Outputs:
- solution: float32 [32, 16, 320, 768], P('gx', 'gy')
The draws below stay inside these ranges and needn't reach their ends.
Inputs may be any that keep to these rules, and one draw needn't show every extreme that they name: `stiffness`: every block is symmetric positive definite. `local_inverse`: every block is symmetric positive definite. `level2_inverse`: every block is symmetric positive definite. `level3_inverse`: symmetric positive definite.
All inputs are finite; a program needn't handle non-finite values.
Results may differ from the reference program's by a relative error of at most 0.0091.
Values may be sent and summed in bfloat16 or wider, within the bound.
No kernel may reach another device: no remote copies, remote signals or barrier semaphores. Data moves between devices by JAX's collectives and lax.ppermute only.
A program may use at most 64 MiB of HBM per device.

```python
import math
import jax
import jax.numpy as jnp
from jax import lax

NRHS = 320
P_SIZE = 8
NAGG = 2
ITERS = 2
M = 768
L2 = 128
L3 = 512
N_GX = 32
N_GY = 16


def spd_blocks(key, lead, order, salt):
    base = jax.random.fold_in(key, salt)
    first, second = jax.random.split(base)
    noise = jax.random.normal(first, lead + (order, order), jnp.float32)
    sym = (noise + jnp.swapaxes(noise, -1, -2)) * (0.35 / (2.0 * math.sqrt(order)))
    diag = jax.random.uniform(second, lead + (order,), jnp.float32, 1.0, 2.0)
    return sym + diag[..., None] * jnp.eye(order, dtype=jnp.float32)


def draw_stiffness(key, part):
    return spd_blocks(key, (N_GX, N_GY), M, 11).astype(jnp.bfloat16)


def draw_local_inverse(key, part):
    return spd_blocks(key, (N_GX, N_GY), M, 23).astype(jnp.bfloat16)


def draw_level2_inverse(key, part):
    return spd_blocks(key, (N_GX,), L2, 37)


def draw_level3_inverse(key, part):
    return spd_blocks(key, (), L3, 41).astype(jnp.bfloat16)


def touch_ends(result, stream_key, low, top_value):
    dims = result.shape
    index_at = [jax.random.randint(jax.random.fold_in(stream_key, axis), (), 0, dims[axis]) for axis in range(len(dims))]
    result = result.at[tuple(index_at)].set(low)
    longest = dims.index(max(dims))
    index_at[longest] = (index_at[longest] + 1) % dims[longest]
    return result.at[tuple(index_at)].set(top_value)


def shard_levels(stream_key, shape, pieces, smallest, largest):
    loudness = 1.0
    for dim, blocks in pieces:
        steps = jax.random.uniform(jax.random.fold_in(jax.random.fold_in(stream_key, 6), dim), (blocks,), jnp.float32, smallest / len(pieces), largest / len(pieces))
        loudness = loudness * jnp.repeat(jnp.exp(steps), shape[dim] // blocks).reshape((-1,) + (1,) * (len(shape) - 1 - dim))
    return loudness


def bell_draw(rng, dims, spread, bound, cuts=(), kind=jnp.bfloat16):
    values = spread * jax.random.normal(rng, dims, jnp.float32)
    if cuts:
        values = values * shard_levels(rng, dims, cuts, -0.22, 0.18)
    return jnp.clip(values, -bound, bound).astype(kind)


def setup_inputs(seed: int = 0) -> dict:
    key_list = jax.random.split(jax.random.key(seed), 8)
    return {
        "load": bell_draw(key_list[0], (N_GX, N_GY, NRHS, M), 1.0, 6.0, ((0, 32), (1, 16)), jnp.float32),
        "stiffness": draw_stiffness(jax.random.fold_in(key_list[7], 71), 0),
        "local_inverse": draw_local_inverse(jax.random.fold_in(key_list[7], 71), 0),
        "phi": bell_draw(key_list[3], (N_GX, N_GY, P_SIZE, M), 0.16, 2.5, ((0, 32), (1, 16)), jnp.float32),
        "level2_inverse": draw_level2_inverse(jax.random.fold_in(key_list[7], 71), 0),
        "level3_inverse": draw_level3_inverse(jax.random.fold_in(key_list[7], 71), 0),
        "aggregate": touch_ends(jax.random.randint(key_list[6], (N_GX, N_GY), 0, NAGG), jax.random.fold_in(key_list[6], 1), 0, NAGG - 1).astype(jnp.int32),
    }


HIGH = lax.Precision.HIGHEST


def assemble(vec):
    width = M // 4
    edges = vec.reshape(N_GX, N_GY, NRHS, 4, width)
    west, east, south, north = edges[..., 0, :], edges[..., 1, :], edges[..., 2, :], edges[..., 3, :]
    new_west = west + jnp.concatenate([jnp.zeros_like(east[:1]), east[:-1]], axis=0)
    new_east = east + jnp.concatenate([west[1:], jnp.zeros_like(west[:1])], axis=0)
    new_south = south + jnp.concatenate([jnp.zeros_like(north[:, :1]), north[:, :-1]], axis=1)
    new_north = north + jnp.concatenate([south[:, 1:], jnp.zeros_like(south[:, :1])], axis=1)
    return jnp.stack([new_west, new_east, new_south, new_north], axis=3).reshape(N_GX, N_GY, NRHS, M)


def make_weights():
    width = M // 4
    col = jnp.broadcast_to(jnp.arange(N_GX, dtype=jnp.int32)[:, None], (N_GX, N_GY))
    row = jnp.broadcast_to(jnp.arange(N_GY, dtype=jnp.int32)[None, :], (N_GX, N_GY))
    edge_w = jnp.stack([jnp.where(col > 0, 0.5, 1.0), jnp.where(col < N_GX - 1, 0.5, 1.0),
                        jnp.where(row > 0, 0.5, 1.0), jnp.where(row < N_GY - 1, 0.5, 1.0)], axis=-1).astype(jnp.float32)
    return jnp.repeat(edge_w, width, axis=-1)[:, :, None, :]


def reference(load, stiffness, local_inverse, phi, level2_inverse, level3_inverse, aggregate):
    stiff32 = stiffness.astype(jnp.float32)
    inverse32 = local_inverse.astype(jnp.float32)
    top32 = level3_inverse.astype(jnp.float32)
    weights = make_weights()
    onehot = (aggregate[:, :, None] == jnp.arange(NAGG, dtype=jnp.int32)).astype(jnp.float32)

    def apply(vec):
        rounded = lax.optimization_barrier(vec.astype(jnp.bfloat16)).astype(jnp.float32)
        return assemble(jnp.einsum('abrm,abnm->abrn', rounded, stiff32, precision=HIGH))

    def precondition(resid):
        scaled = weights * resid
        rounded = lax.optimization_barrier(scaled.astype(jnp.bfloat16)).astype(jnp.float32)
        local = jnp.einsum('abrm,abnm->abrn', rounded, inverse32, precision=HIGH)
        primal = jnp.einsum('abrm,abpm->abrp', scaled, phi, precision=HIGH)
        grouped = primal.transpose(0, 2, 1, 3).reshape(N_GX, NRHS, L2)
        second = jnp.einsum('grk,glk->grl', grouped, level2_inverse, precision=HIGH)
        second = second.reshape(N_GX, NRHS, N_GY, P_SIZE).transpose(0, 2, 1, 3)
        summed = jnp.einsum('gbq,gbrp->grqp', onehot, primal, precision=HIGH)
        summed = summed.transpose(1, 0, 2, 3).reshape(NRHS, L3)
        summed = lax.optimization_barrier(summed.astype(jnp.bfloat16)).astype(jnp.float32)
        third = jnp.einsum('rl,kl->rk', summed, top32, precision=HIGH).reshape(NRHS, N_GX, NAGG, P_SIZE)
        third = jnp.einsum('gbq,rgqp->gbrp', onehot, third, precision=HIGH)
        full = local + jnp.einsum('abrp,abpm->abrm', second + third, phi, precision=HIGH)
        return assemble(weights * full)

    def inner(left, right):
        return jnp.sum(weights * left * right, axis=(0, 1, 3))

    rhs = assemble(load)
    solution = jnp.zeros_like(rhs)
    resid = rhs
    zvec = precondition(resid)
    svec = apply(zvec)
    pvec = zvec
    gamma = inner(resid, zvec)
    alpha = gamma / inner(pvec, svec)
    for step in range(ITERS):
        solution = solution + alpha[:, None] * pvec
        resid = resid - alpha[:, None] * svec
        if step < ITERS - 1:
            zvec = precondition(resid)
            wvec = apply(zvec)
            newer = inner(resid, zvec)
            beta = newer / gamma
            pvec = zvec + beta[:, None] * pvec
            svec = wvec + beta[:, None] * svec
            alpha = newer / inner(pvec, svec)
            gamma = newer
    return solution
```

```python
import jax
import jax.numpy as jnp
from jax import lax
from jax.sharding import Mesh
from jax.sharding import PartitionSpec as P

NAGG = 2
GX = ("gx_0", "gx_1")
GY = ("gy_0", "gy_1")
PLANE = ("gx_1", "gy_0", "gy_1")
DEPTH = ("gx_0",)

HIGH = lax.Precision.HIGHEST


def from_behind(value, axis, steps):
    count = lax.axis_size(axis)
    first, last = (max(0, -steps), min(count, count - steps))
    return lax.ppermute(value, axis, [(source, source + steps) for source in range(first, last)])


def exchange(parts, axis):
    return lax.all_to_all(parts, axis, split_axis=0, concat_axis=0, tiled=True)


def copies(value, axis):
    return exchange(jnp.broadcast_to(value, (lax.axis_size(axis), *value.shape)), axis)


def assemble(vec):
    width = vec.shape[0] // 4
    west, east, south, north = (vec[k * width : (k + 1) * width] for k in range(4))
    narrow = vec.astype(jnp.bfloat16)
    west_n, east_n, south_n, north_n = (narrow[k * width : (k + 1) * width] for k in range(4))
    new_west = west + from_behind(east_n, GX, 1).astype(vec.dtype)
    new_east = east + from_behind(west_n, GX, -1).astype(vec.dtype)
    new_south = south + from_behind(north_n, GY, 1).astype(vec.dtype)
    new_north = north + from_behind(south_n, GY, -1).astype(vec.dtype)
    return jnp.concatenate([new_west, new_east, new_south, new_north], axis=0)


def halves(value):
    upper = lax.reduce_precision(value, 8, 7)
    return (upper.astype(jnp.bfloat16), (value - upper).astype(jnp.bfloat16))


def times(left, right):
    return lax.dot_general(
        left, right, (((1,), (0,)), ((), ())), preferred_element_type=jnp.float32
    )


def times_high(left, right):
    return lax.dot_general(
        left,
        right,
        (((1,), (0,)), ((), ())),
        precision=HIGH,
        preferred_element_type=jnp.float32,
    )


def body(load, stiffness, local_inverse, phi, level2_inverse, level3_inverse, aggregate):
    load_here = load[0, 0].T
    stiff = stiffness[0, 0]
    inverse = local_inverse[0, 0]
    basis = phi[0, 0]
    second_inv = level2_inverse[0]
    total, rows = load_here.shape
    width = total // 4
    count = basis.shape[0]
    block = NAGG * count
    col = lax.axis_index(GX)
    row = lax.axis_index(GY)
    cols_total = lax.axis_size(GX)
    rows_total = lax.axis_size(GY)
    share = rows // rows_total
    edge_w = jnp.stack(
        [
            jnp.where(col > 0, 0.5, 1.0),
            jnp.where(col < cols_total - 1, 0.5, 1.0),
            jnp.where(row > 0, 0.5, 1.0),
            jnp.where(row < rows_total - 1, 0.5, 1.0),
        ]
    ).astype(jnp.float32)
    weights = jnp.repeat(edge_w, width)[:, None]
    own = aggregate[0, 0]
    mine = lax.dynamic_slice_in_dim(level3_inverse, col * block, block, 0).astype(jnp.float32)
    basis_hi, basis_lo = halves(basis)
    spread = jnp.concatenate([basis_hi, basis_lo, basis_hi], axis=0).T

    def scatter(value):
        lead = value.shape[0]
        parts = value.reshape(lead, rows_total, share).transpose(1, 0, 2)
        return exchange(parts, GY)

    def gather(parts):
        back = exchange(parts, GY)
        return back.transpose(1, 0, 2).reshape(back.shape[1], rows)

    def precondition(scaled, extra):
        primal = times_high(basis, scaled)
        masked = [jnp.where(own == label, primal, 0.0) for label in range(NAGG)]
        kept = 0 if extra is None else extra.shape[0]
        message = jnp.concatenate(masked if extra is None else [*masked, extra], axis=0)
        local = times(inverse, scaled.astype(jnp.bfloat16))
        group = scatter(message)
        grouped = sum(group[:, q * count : (q + 1) * count] for q in range(NAGG))
        grouped = grouped.reshape(rows_total * count, share)
        everyone = copies(jnp.sum(group, axis=0), GX)
        second = times_high(second_inv, grouped).reshape(rows_total, 1, count, share)
        summed = everyone[:, :block].reshape(cols_total * block, share)
        third = times_high(mine, summed).reshape(1, NAGG, count, share)
        answer = (second + third).reshape(rows_total, block, share)
        if kept:
            sums = jnp.sum(everyone[:, block:], axis=0)
            sums = jnp.broadcast_to(sums, (rows_total, kept, share))
            answer = jnp.concatenate([answer, sums], axis=1)
        result = gather(answer)
        coarse = result[:count]
        for label in range(1, NAGG):
            coarse = jnp.where(own == label, result[label * count : (label + 1) * count], coarse)
        coarse_hi, coarse_lo = halves(coarse)
        stacked = jnp.concatenate([coarse_hi, coarse_hi, coarse_lo], axis=0)
        full = local + times(spread, stacked)
        return (assemble(weights * full), result[block:])

    def apply(vec):
        return times(stiff, vec.astype(jnp.bfloat16))

    def inner(left, right):
        return jnp.sum(left * right, axis=0)

    rhs = weights * assemble(load_here)
    zero, _ = precondition(rhs, None)
    image = apply(zero)
    dots = jnp.stack([inner(rhs, zero), inner(zero, image)])
    scaled = weights * assemble(image)
    other, dots = precondition(scaled, dots)
    gamma, delta = (dots[0], dots[1])
    alpha = gamma / delta
    one = zero - alpha * other
    resid = rhs - alpha * scaled
    partial = jnp.stack([inner(resid, one), inner(one, apply(one))])
    partial = jnp.sum(copies(partial, PLANE), axis=0)
    partial = jnp.sum(copies(partial, DEPTH), axis=0)
    newer, delta = (partial[0], partial[1])
    beta = newer / gamma
    step = newer / (delta - beta * newer / alpha)
    result = (alpha + step * beta) * zero + step * one
    return result.T[None, None]


def solution(mesh):
    finer = Mesh(mesh.devices.reshape(16, 2, 4, 4), ("gx_0", "gx_1", "gy_0", "gy_1"))
    return jax.shard_map(
        body,
        mesh=finer,
        in_specs=(
            P(GX, GY, None, None),
            P(GX, GY, None, None),
            P(GX, GY, None, None),
            P(GX, GY, None, None),
            P(GX, None, None),
            P(),
            P(GX, GY),
        ),
        out_specs=P(GX, GY, None, None),
        check_vma=False,
    )
```

```python
import jax
import jax.numpy as jnp
from jax import lax
from jax.sharding import Mesh
from jax.sharding import PartitionSpec as P

NAGG = 2
GX = ("gx_0", "gx_1")
GY = ("gy_0", "gy_1")
CORE = ("gx_1",)
PLANE = ("gx_1", "gy_0", "gy_1")
DEPTH = ("gx_0",)

HIGH = lax.Precision.HIGHEST


def traded(value, axis, first):
    count = lax.axis_size(axis)
    pairs = [(k, k + 1) for k in range(first, count - 1, 2)]
    return lax.ppermute(value, axis, pairs + [(b, a) for a, b in pairs])


def copies(value, axis):
    parts = jnp.broadcast_to(value, (lax.axis_size(axis), *value.shape))
    return lax.all_to_all(parts, axis, split_axis=0, concat_axis=0, tiled=True)


def edges_of(vec):
    width = vec.shape[0] // 4
    return [vec[k * width : (k + 1) * width] for k in range(4)]


def neighbours(parts):
    west, east, south, north = parts
    left = lax.axis_index(GX) % 2 == 0
    lower = lax.axis_index(GY) % 2 == 0
    far_y = traded(jnp.where(lower, south, north), GY, 1)
    near_y = traded(jnp.where(lower, north, south), GY, 0)
    far_x = traded(jnp.where(left, west, east), GX, 1)
    near_x = traded(jnp.where(left, east, west), GX, 0)
    return (
        jnp.where(left, far_x, near_x),
        jnp.where(left, near_x, far_x),
        jnp.where(lower, far_y, near_y),
        jnp.where(lower, near_y, far_y),
    )


def assemble(vec):
    others = neighbours(edges_of(vec.astype(jnp.bfloat16)))
    return jnp.concatenate(
        [mine + other.astype(vec.dtype) for mine, other in zip(edges_of(vec), others)], axis=0
    )


def halves(value):
    upper = lax.reduce_precision(value, 8, 7)
    return (upper.astype(jnp.bfloat16), (value - upper).astype(jnp.bfloat16))


def times(left, right):
    return lax.dot_general(
        left, right, (((1,), (0,)), ((), ())), preferred_element_type=jnp.float32
    )


def times_high(left, right):
    return lax.dot_general(
        left,
        right,
        (((1,), (0,)), ((), ())),
        precision=HIGH,
        preferred_element_type=jnp.float32,
    )


def body(load, stiffness, local_inverse, phi, level2_inverse, level3_inverse, aggregate):
    load_here = load[0, 0].T
    stiff = stiffness[0, 0]
    inverse = local_inverse[0, 0]
    basis = phi[0, 0]
    total, rows = load_here.shape
    width = total // 4
    count = basis.shape[0]
    block = NAGG * count
    col = lax.axis_index(GX)
    row = lax.axis_index(GY)
    core = lax.axis_index(CORE)
    cols_total = lax.axis_size(GX)
    rows_total = lax.axis_size(GY)
    cores = lax.axis_size(CORE)
    edge_w = jnp.stack(
        [
            jnp.where(col > 0, 0.5, 1.0),
            jnp.where(col < cols_total - 1, 0.5, 1.0),
            jnp.where(row > 0, 0.5, 1.0),
            jnp.where(row < rows_total - 1, 0.5, 1.0),
        ]
    ).astype(jnp.float32)
    weights = jnp.repeat(edge_w, width)[:, None]
    own = aggregate[0, 0]
    second_inv = lax.dynamic_slice_in_dim(level2_inverse[0], row * count, count, 0)
    third_inv = lax.dynamic_slice_in_dim(
        level3_inverse, (col - core) * block, cores * block, 0
    )
    third_inv = third_inv.reshape(cores * block, cols_total // cores, cores, block)
    third_inv = lax.dynamic_index_in_dim(third_inv, core, 2, keepdims=False)
    planes = cols_total // cores
    third_first = third_inv.reshape(cores * block, planes * block)
    adders = jnp.array([[1, 0, 1, 0, 0, 0, 0, 0], [0, 1, 0, 1, 0, 0, 0, 0]], jnp.bfloat16)
    adders = jnp.pad(adders, ((0, 6), (block, 0)))
    third_dots = jnp.concatenate(
        [
            jnp.pad(third_inv, ((0, 0), (0, 0), (0, 8))),
            jnp.broadcast_to(adders[:, None], (8, planes, block + 8)),
        ],
        axis=0,
    ).reshape(-1, planes * (block + 8))
    basis_hi, basis_lo = halves(basis)
    spread = jnp.concatenate([basis_hi, basis_lo, basis_hi], axis=0).T
    tags = jnp.broadcast_to(own.astype(jnp.float32), (count, 128 - rows % 128))

    def swapped(value):
        return lax.ppermute(value, CORE, [(0, 1), (1, 0)])

    def precondition(scaled, extra, members):
        primal = times_high(basis, scaled)
        local = times(inverse, scaled.astype(jnp.bfloat16))
        if members is None:
            group = copies(jnp.concatenate([primal, tags], axis=1), GY)
            members = group[:, :1, rows : rows + 1]
            group = group[:, :, :rows]
        else:
            group = copies(jnp.concatenate([primal, extra], axis=0), GY)
        group, found = (group[:, :count], group[:, count:])
        summed = [
            jnp.sum(jnp.where(members == label, group, 0.0), axis=0) for label in range(NAGG)
        ]
        third_inv = third_first
        if extra is not None:
            found = jnp.sum(found, axis=0)
            upper = lax.reduce_precision(found, 8, 7)
            at = lax.broadcasted_iota(jnp.int32, found.shape, 0)
            summed.append(jnp.where(at < 2, upper, jnp.where(at < 4, found - upper, 0.0)))
            third_inv = third_dots
        everyone = copies(jnp.concatenate(summed, axis=0).astype(jnp.bfloat16), DEPTH)
        second = times_high(second_inv, group.reshape(rows_total * count, rows))
        parts = times(third_inv, everyone.reshape(-1, rows))
        here, there = (parts[:block], parts[block : 2 * block])
        kept = jnp.where(core == 0, here, there)
        sent = jnp.where(core == 0, there, here)
        dots = parts[2 * block :]
        got = swapped(jnp.concatenate([sent, dots], axis=0))
        third = kept + got[:block]
        third_own = third[:count]
        for label in range(1, NAGG):
            third_own = jnp.where(own == label, third[label * count : (label + 1) * count], third_own)
        coarse_hi, coarse_lo = halves(second + third_own)
        stacked = jnp.concatenate([coarse_hi, coarse_hi, coarse_lo], axis=0)
        full = local + times(spread, stacked)
        return (assemble(weights * full), members, dots + got[block:])

    def apply(vec):
        return times(stiff, vec.astype(jnp.bfloat16))

    def inner(left, right):
        return jnp.sum(left * right, axis=0)

    rhs = weights * assemble(load_here)
    zero, members, _ = precondition(rhs, None, None)
    image = apply(zero)
    dots = jnp.stack([inner(rhs, zero), inner(zero, image)])
    dots = jnp.concatenate([dots, dots, jnp.zeros((4, rows), jnp.float32)], axis=0)
    scaled = weights * assemble(image)
    other, _, dots = precondition(scaled, dots, members)
    gamma, delta = (dots[0], dots[1])
    alpha = gamma / delta
    one = zero - alpha * other
    resid = rhs - alpha * scaled
    partial = jnp.stack([inner(resid, one), inner(one, apply(one))])
    partial = jnp.sum(copies(partial, PLANE), axis=0)
    partial = jnp.sum(copies(partial, DEPTH), axis=0)
    newer, delta = (partial[0], partial[1])
    beta = newer / gamma
    step = newer / (delta - beta * newer / alpha)
    result = (alpha + step * beta) * zero + step * one
    return result.T[None, None]


def solution(mesh):
    finer = Mesh(mesh.devices.reshape(16, 2, 4, 4), ("gx_0", "gx_1", "gy_0", "gy_1"))
    return jax.shard_map(
        body,
        mesh=finer,
        in_specs=(
            P(GX, GY, None, None),
            P(GX, GY, None, None),
            P(GX, GY, None, None),
            P(GX, GY, None, None),
            P(GX, None, None),
            P(),
            P(GX, GY),
        ),
        out_specs=P(GX, GY, None, None),
        check_vma=False,
    )
```

```python
import jax
import jax.numpy as jnp
from jax import lax
from jax.sharding import Mesh
from jax.sharding import PartitionSpec as P

NAGG = 2
GX = ("gx_0", "gx_1")
GY = ("gy_0", "gy_1")
CORE = ("gx_1",)
PLANE = ("gx_1", "gy_0", "gy_1")
DEPTH = ("gx_0",)

HIGH = lax.Precision.HIGHEST


def traded(value, axis, first):
    count = lax.axis_size(axis)
    pairs = [(k, k + 1) for k in range(first, count - 1, 2)]
    return lax.ppermute(value, axis, pairs + [(b, a) for a, b in pairs])


def copies(value, axis):
    parts = jnp.broadcast_to(value, (lax.axis_size(axis), *value.shape))
    return lax.all_to_all(parts, axis, split_axis=0, concat_axis=0, tiled=True)


def edges_of(vec):
    width = vec.shape[0] // 4
    return [vec[k * width : (k + 1) * width] for k in range(4)]


def beside_x(west, east):
    left = lax.axis_index(GX) % 2 == 0
    far = traded(jnp.where(left, west, east), GX, 1)
    near = traded(jnp.where(left, east, west), GX, 0)
    return (jnp.where(left, far, near), jnp.where(left, near, far))


def beside_y(south, north):
    lower = lax.axis_index(GY) % 2 == 0
    far = traded(jnp.where(lower, south, north), GY, 1)
    near = traded(jnp.where(lower, north, south), GY, 0)
    return (jnp.where(lower, far, near), jnp.where(lower, near, far))


def joined(vec, others):
    return jnp.concatenate(
        [mine + other.astype(vec.dtype) for mine, other in zip(edges_of(vec), others)], axis=0
    )


def assemble(vec):
    west, east, south, north = edges_of(vec.astype(jnp.bfloat16))
    y = beside_y(south, north)
    return joined(vec, (*beside_x(west, east), *y))


def halves(value):
    upper = lax.reduce_precision(value, 8, 7)
    return (upper.astype(jnp.bfloat16), (value - upper).astype(jnp.bfloat16))


def times(left, right):
    return lax.dot_general(
        left, right, (((1,), (0,)), ((), ())), preferred_element_type=jnp.float32
    )


def times_high(left, right):
    return lax.dot_general(
        left,
        right,
        (((1,), (0,)), ((), ())),
        precision=HIGH,
        preferred_element_type=jnp.float32,
    )


def body(load, stiffness, local_inverse, phi, level2_inverse, level3_inverse, aggregate):
    load_here = load[0, 0].T
    stiff = stiffness[0, 0]
    inverse = local_inverse[0, 0]
    basis = phi[0, 0]
    total, rows = load_here.shape
    width = total // 4
    count = basis.shape[0]
    block = NAGG * count
    col = lax.axis_index(GX)
    row = lax.axis_index(GY)
    core = lax.axis_index(CORE)
    cols_total = lax.axis_size(GX)
    rows_total = lax.axis_size(GY)
    cores = lax.axis_size(CORE)
    edge_w = jnp.stack(
        [
            jnp.where(col > 0, 0.5, 1.0),
            jnp.where(col < cols_total - 1, 0.5, 1.0),
            jnp.where(row > 0, 0.5, 1.0),
            jnp.where(row < rows_total - 1, 0.5, 1.0),
        ]
    ).astype(jnp.float32)
    weights = jnp.repeat(edge_w, width)[:, None]
    own = aggregate[0, 0]
    before, after = (jnp.maximum(row - 1, 0), jnp.minimum(row + 1, rows_total - 1))
    second_inv = jnp.concatenate(
        [
            lax.dynamic_slice_in_dim(level2_inverse[0], k * count, count, 0)
            for k in (row, before, after)
        ],
        axis=0,
    )
    planes = cols_total // cores
    columns = level3_inverse.reshape(cols_total * block, planes, cores, block)
    columns = lax.dynamic_index_in_dim(columns, core, 2, keepdims=False)
    left = jnp.maximum(col - core - 1, 0)
    right = jnp.minimum(col - core + cores, cols_total - 1)
    third_inv = jnp.concatenate(
        [
            lax.dynamic_slice_in_dim(columns, left * block, block, 0),
            lax.dynamic_slice_in_dim(columns, (col - core) * block, cores * block, 0),
            lax.dynamic_slice_in_dim(columns, right * block, block, 0),
        ],
        axis=0,
    )
    near = (cores + 1) * block
    third_first = third_inv.reshape(-1, planes * block)
    adders = jnp.array([[1, 0, 1, 0, 0, 0, 0, 0], [0, 1, 0, 1, 0, 0, 0, 0]], jnp.bfloat16)
    adders = jnp.pad(adders, ((0, 6), (block, 0)))
    third_dots = jnp.concatenate(
        [
            jnp.pad(third_inv, ((0, 0), (0, 0), (0, 8))),
            jnp.broadcast_to(adders[:, None], (8, planes, block + 8)),
        ],
        axis=0,
    ).reshape(-1, planes * (block + 8))
    basis_hi, basis_lo = halves(basis)
    spread = jnp.concatenate([basis_hi, basis_lo, basis_hi], axis=0).T
    tags = jnp.broadcast_to(own.astype(jnp.float32), (count, 128 - rows % 128))
    label = jnp.broadcast_to(own.astype(jnp.bfloat16), (total, 8))
    depth = spread.shape[1]
    first = jnp.concatenate([load_here.astype(jnp.bfloat16), spread, label], axis=1)
    west, east, south, north = edges_of(first)
    others_y = beside_y(south, north)
    others = (*beside_x(west, east), *others_y)
    rhs = weights * joined(load_here, [other[:, :rows] for other in others])
    west_own, east_own = (other[0, rows + depth].astype(jnp.int32) for other in others[:2])
    across = jnp.concatenate([other[:, rows : rows + depth] for other in others], axis=0)
    edge_at = lax.broadcasted_iota(jnp.int32, (total, depth), 0) // width
    lift = jnp.concatenate(
        [spread, *(jnp.where(edge_at == k, across, jnp.zeros_like(across)) for k in range(4))],
        axis=1,
    )

    def chosen(third, at, agg):
        value = third[at : at + count]
        for k in range(1, NAGG):
            value = jnp.where(agg == k, third[at + k * count : at + (k + 1) * count], value)
        return value

    def swapped(value):
        return lax.ppermute(value, CORE, [(0, 1), (1, 0)])

    def precondition(scaled, extra, members):
        primal = times_high(basis, scaled)
        local = times(inverse, scaled.astype(jnp.bfloat16))
        if members is None:
            group = copies(jnp.concatenate([primal, tags], axis=1), GY)
            members = group[:, :1, rows : rows + 1]
            group = group[:, :, :rows]
        else:
            group = copies(jnp.concatenate([primal, extra], axis=0), GY)
        west, east, south, north = edges_of(local.astype(jnp.bfloat16))
        others_y = beside_y(south, north)
        group, found = (group[:, :count], group[:, count:])
        summed = [
            jnp.sum(jnp.where(members == label, group, 0.0), axis=0) for label in range(NAGG)
        ]
        third_inv = third_first
        if extra is not None:
            found = jnp.sum(found, axis=0)
            upper = lax.reduce_precision(found, 8, 7)
            at = lax.broadcasted_iota(jnp.int32, found.shape, 0)
            summed.append(jnp.where(at < 2, upper, jnp.where(at < 4, found - upper, 0.0)))
            third_inv = third_dots
        everyone = copies(jnp.concatenate(summed, axis=0).astype(jnp.bfloat16), DEPTH)
        second = times_high(second_inv, group.reshape(rows_total * count, rows))
        parts = times(third_inv, everyone.reshape(-1, rows))
        second_hi, second_lo = halves(second[:count])
        others_x = beside_x(
            jnp.concatenate([west, second_hi, second_lo], axis=0),
            jnp.concatenate([east, second_hi, second_lo], axis=0),
        )
        second_west, second_east = (
            (other[width : width + count].astype(jnp.float32) + other[width + count :].astype(jnp.float32))
            for other in others_x
        )
        local = joined(local, (*(other[:width] for other in others_x), *others_y))
        dots = parts[near + block :]
        kept = jnp.where(core == 0, parts[:near], parts[block : near + block])
        sent = jnp.where(core == 0, parts[block : near + block], parts[:near])
        got = swapped(jnp.concatenate([sent, dots], axis=0))
        third = kept + got[:near]
        aggs = members[:, 0, 0]
        coarse = [
            second[:count] + chosen(third, block, own),
            second_west + chosen(third, 0, west_own),
            second_east + chosen(third, 2 * block, east_own),
            second[count : 2 * count] + chosen(third, block, aggs[before]),
            second[2 * count :] + chosen(third, block, aggs[after]),
        ]
        coarse_hi, coarse_lo = halves(jnp.stack(coarse))
        stacked = jnp.concatenate([coarse_hi, coarse_hi, coarse_lo], axis=1)
        full = local + times(lift, stacked.reshape(5 * depth, rows))
        return (weights * full, members, dots + got[near:])

    def apply(vec):
        return times(stiff, vec.astype(jnp.bfloat16))

    def inner(left, right):
        return jnp.sum(left * right, axis=0)

    zero, members, _ = precondition(rhs, None, None)
    image = apply(zero)
    dots = jnp.stack([inner(rhs, zero), inner(zero, image)])
    dots = jnp.concatenate([dots, dots, jnp.zeros((4, rows), jnp.float32)], axis=0)
    scaled = weights * assemble(image)
    other, _, dots = precondition(scaled, dots, members)
    gamma, delta = (dots[0], dots[1])
    alpha = gamma / delta
    one = zero - alpha * other
    resid = rhs - alpha * scaled
    partial = jnp.stack([inner(resid, one), inner(one, apply(one))])
    partial = jnp.sum(copies(partial, PLANE), axis=0)
    partial = jnp.sum(copies(partial, DEPTH), axis=0)
    newer, delta = (partial[0], partial[1])
    beta = newer / gamma
    step = newer / (delta - beta * newer / alpha)
    result = (alpha + step * beta) * zero + step * one
    return result.T[None, None]


def solution(mesh):
    finer = Mesh(mesh.devices.reshape(16, 2, 4, 4), ("gx_0", "gx_1", "gy_0", "gy_1"))
    return jax.shard_map(
        body,
        mesh=finer,
        in_specs=(
            P(GX, GY, None, None),
            P(GX, GY, None, None),
            P(GX, GY, None, None),
            P(GX, GY, None, None),
            P(GX, None, None),
            P(),
            P(GX, GY),
        ),
        out_specs=P(GX, GY, None, None),
        check_vma=False,
    )
```
